256 devices in a mesh: row: 64 (over x, y, z_hi, core), col: 4 (over z_lo).
Axes of the slice: x: 4, y: 4, z: 8 (z_hi: 2, z_lo: 4; z = z_hi * 4 + z_lo), core: 2. Of those that a mesh axis runs over, the one named last changes fastest.
Arguments:
- sweep_start: int32 [8], replicated, may hold values from 1 to 63, as said below
- block_len: int32 [8, 256], P(None, 'row'), may hold values from 64 to 128, as said below
- reflectors: float32 [8, 256, 128, 64], P('col', 'row'), may hold values from -8 to 8, as said below
- tfactors: float32 [8, 256, 64, 64], P('col', 'row'), may hold values from -2 to 2, as said below
- panel: float32 [32768, 128], P('row'), may hold values from -180 to 180
- eigvecs: float32 [32768, 2048], P('row', 'col'), may hold values from -4 to 4
Outputs:
- result: float32 [32768, 2048], P('row', 'col')
The draws below stay inside these ranges and needn't reach their ends.
Inputs may be any that keep to these rules, and one draw needn't show every extreme that they name: `sweep_start`: some sweep starts at row 63. In the last block of each sweep, sweep_start plus block_len is at most 128. `reflectors`: each block's vectors are unit lower trapezoidal: entry (k, k) is 1 and entries above it are 0. tfactors[s, b] is the triangular factor that makes the block a product of Householder reflections of its masked vectors.
All inputs are finite; a program needn't handle non-finite values.
Results may differ from the reference program's by a relative error of at most 0.0003.
Values sent between devices are 32-bit elements; how exact they have to be, the bound alone decides.
No kernel may reach another device: no remote copies, remote signals or barrier semaphores. Data moves between devices by JAX's collectives and lax.ppermute only.
A program may use at most 64 MiB of HBM per device.

```python
import jax
import jax.numpy as jnp
from jax import lax

ROWS = 512
BAND = 128
KREF = 64
WANTED = 2048
SWEEPS = 8
ORDER = 32768
N_ROW = 64


def sweep_layout(key):
    base = jax.random.fold_in(key, 11)
    key_start, key_widest, key_length, key_device = jax.random.split(base, 4)
    block_total = ROWS // BAND * N_ROW
    starts = jax.random.randint(key_start, (SWEEPS,), 1, BAND // 2)
    widest = jax.random.randint(key_widest, (), 0, SWEEPS)
    sweep_ids = jnp.arange(SWEEPS)
    starts = jnp.where(sweep_ids == widest, BAND // 2 - 1, starts)
    lengths = jax.random.randint(key_length, (SWEEPS, block_total), KREF, BAND + 1)
    device = jax.random.randint(key_device, (), 0, N_ROW - 1)
    target = device * (ROWS // BAND) + ROWS // BAND - 1
    block_ids = jnp.arange(block_total)
    hit = (sweep_ids[:, None] == widest) & (block_ids[None, :] == target)
    lengths = jnp.where(hit, BAND, lengths)
    capped = jnp.minimum(lengths[:, block_total - 1], BAND - starts)
    lengths = lengths.at[:, block_total - 1].set(capped)
    return (starts.astype(jnp.int32), lengths.astype(jnp.int32))


def invert_batch(upper):
    width = upper.shape[-1]
    diagonal = jnp.diagonal(upper, axis1=-2, axis2=-1)
    scaled = upper / diagonal[..., :, None]
    identity = jnp.eye(width, dtype=jnp.float32)
    strict = scaled - identity
    solved = jnp.zeros_like(upper)

    def sweep_row(counter, current):
        row_id = width - 1 - counter
        strict_row = lax.dynamic_slice_in_dim(strict, row_id, 1, axis=strict.ndim - 2)
        unit_row = lax.dynamic_slice_in_dim(identity, row_id, 1, axis=0)
        known = jnp.einsum('...ij,...jk->...ik', strict_row, current, precision=lax.Precision.HIGHEST)
        new_row = unit_row - known
        return lax.dynamic_update_slice_in_dim(current, new_row, row_id, axis=current.ndim - 2)
    solved = lax.fori_loop(0, width, sweep_row, solved)
    return solved / diagonal[..., None, :]


def reflector_set(key):
    starts, lengths = sweep_layout(key)
    block_total = ROWS // BAND * N_ROW
    key_values = jax.random.fold_in(jax.random.fold_in(key, 23), 0)
    shape = (SWEEPS, block_total, BAND, KREF)
    values = 0.5 * jax.random.truncated_normal(key_values, -4.0, 4.0, shape, jnp.float32)
    row_ids = jnp.arange(BAND)[:, None]
    col_ids = jnp.arange(KREF)[None, :]
    below = (row_ids > col_ids).astype(jnp.float32)
    diagonal = (row_ids == col_ids).astype(jnp.float32)
    norm_scale = lax.rsqrt(lengths.astype(jnp.float32))[:, :, None, None]
    values = values * norm_scale * below + diagonal
    row_mask = (jnp.arange(BAND)[None, None, :] < lengths[:, :, None]).astype(jnp.float32)
    masked = values * row_mask[..., None]
    gram = jnp.einsum('sjbk,sjbl->sjkl', masked, masked, precision=lax.Precision.HIGHEST)
    identity = jnp.eye(KREF, dtype=jnp.float32)
    upper_form = jnp.triu(gram, 1) + 0.5 * gram * identity
    factors = invert_batch(upper_form)
    return (values, factors)


def vector_set(key):
    base = jax.random.fold_in(key, 37)
    key_vectors, key_noise, key_columns, key_scale = jax.random.split(base, 4)
    vectors = jax.random.truncated_normal(key_vectors, -4.0, 4.0, (ORDER, WANTED), jnp.float32)
    spread = 10.0
    columns = jax.random.permutation(key_columns, WANTED)[:BAND]
    noise = jax.random.truncated_normal(key_noise, -4.0, 4.0, (ORDER, BAND), jnp.float32)
    scales = jnp.exp(jax.random.uniform(key_scale, (ORDER, 1), jnp.float32, 0.0, jnp.log(spread)))
    panel = (vectors[:, columns] + 0.5 * noise) * scales
    return (vectors, panel)


def draw_sweep_start(key, part):
    return sweep_layout(key)[0]


def draw_block_len(key, part):
    return sweep_layout(key)[1]


def draw_reflectors(key, part):
    return reflector_set(key)[0]


def draw_tfactors(key, part):
    return reflector_set(key)[1]


def draw_panel(key, part):
    return vector_set(key)[1]


def draw_eigvecs(key, part):
    return vector_set(key)[0]


def setup_inputs(seed: int = 0) -> dict:
    seeds = jax.random.split(jax.random.key(seed), 7)
    return {
        "sweep_start": draw_sweep_start(jax.random.fold_in(seeds[6], 71), 0),
        "block_len": draw_block_len(jax.random.fold_in(seeds[6], 71), 0),
        "reflectors": draw_reflectors(jax.random.fold_in(seeds[6], 71), 0),
        "tfactors": draw_tfactors(jax.random.fold_in(seeds[6], 71), 0),
        "panel": draw_panel(jax.random.fold_in(seeds[6], 71), 0),
        "eigvecs": draw_eigvecs(jax.random.fold_in(seeds[6], 71), 0),
    }


def apply_blocks(window, reflect, triangle):
    highest = lax.Precision.HIGHEST
    projected = jnp.einsum('jbk,jbm->jkm', reflect, window, precision=highest)
    combined = jnp.einsum('jkl,jlm->jkm', triangle, projected, precision=highest)
    return window - jnp.einsum('jbk,jkm->jbm', reflect, combined, precision=highest)

def reference(sweep_start, block_len, reflectors, tfactors, panel, eigvecs):
    highest = lax.Precision.HIGHEST
    block_total = ORDER // BAND
    lane_index = jnp.arange(BAND, dtype=jnp.int32)
    vectors = eigvecs
    for step_index in range(SWEEPS):
        padded = jnp.concatenate([vectors, jnp.zeros((BAND, WANTED), eigvecs.dtype)], axis=0)
        offset = sweep_start[step_index].astype(jnp.int32)
        window = lax.dynamic_slice_in_dim(padded, offset, ORDER, 0).reshape(block_total, BAND, WANTED)
        live_rows = (lane_index[None, :] < block_len[step_index][:, None]).astype(eigvecs.dtype)
        masked = reflectors[step_index] * live_rows[:, :, None]
        window = apply_blocks(window, masked, tfactors[step_index])
        padded = lax.dynamic_update_slice_in_dim(padded, window.reshape(ORDER, WANTED), offset, 0)
        vectors = padded[:ORDER]
    gram_total = lax.dot_general(panel, panel, (((0,), (0,)), ((), ())), precision=highest)
    projection = lax.dot_general(panel, vectors, (((0,), (0,)), ((), ())), precision=highest)
    identity = jnp.eye(BAND, dtype=panel.dtype)
    upper_form = jnp.triu(gram_total, 1) + 0.5 * gram_total * identity
    factor = lax.linalg.triangular_solve(upper_form, identity, left_side=True, lower=False)
    inner = jnp.dot(factor, projection, precision=highest)
    return vectors - jnp.dot(panel, inner, precision=highest)
```

```python
import functools

import jax
import jax.numpy as jnp
from jax import lax
from jax.experimental import pallas as pl
from jax.experimental.pallas import tpu as pltpu
from jax.sharding import PartitionSpec as P

F32 = jnp.float32
BF16 = jnp.bfloat16
BAND = 128
KREF = 64
HALF = 64
ROWS = 512
COLS = 512
ABOVE = BAND
EXT = ABOVE + ROWS + HALF
EXTRA = 2 * KREF * BAND // COLS
DOWN = BAND + EXTRA
VMEM = pl.BlockSpec(memory_space=pltpu.VMEM)
SMEM = pl.BlockSpec(memory_space=pltpu.SMEM)
PARAMS = pltpu.CompilerParams(vmem_limit_bytes=48 * 1024 * 1024)


def halves(value):
    high = value.astype(BF16)
    return high, (value - high.astype(F32)).astype(BF16)


def product(left, right):
    (lh, ll), (rh, rl) = left, right
    dot = functools.partial(jnp.dot, preferred_element_type=F32)
    return dot(lh, rh) + (dot(ll, rh) + dot(lh, rl))


def full_dot(left, right):
    return jnp.dot(left, right, precision=lax.Precision.HIGHEST, preferred_element_type=F32)


def pack_kernel(lens, reflect, factor, out):
    row = lax.broadcasted_iota(jnp.int32, (KREF, BAND), 0)
    lane = lax.broadcasted_iota(jnp.int32, (KREF, BAND), 1)
    below = jnp.zeros((BAND - KREF, KREF), F32)
    for j in range(reflect.shape[0]):
        for b in range(reflect.shape[1]):
            side = jnp.concatenate([factor[j, b], below], axis=0)
            turned = jnp.concatenate([reflect[j, b], side], axis=1).T
            live = jnp.where(lane < lens[j, b], turned[:KREF], 0.0)
            out[j, b] = jnp.where(lane > row, live, turned[KREF:])


def pack(lens, reflect, factor):
    shape = (*reflect.shape[:2], KREF, BAND)
    return pl.pallas_call(
        pack_kernel,
        out_shape=jax.ShapeDtypeStruct(shape, F32),
        in_specs=[SMEM, VMEM, VMEM],
        out_specs=VMEM,
        compiler_params=PARAMS,
        name="pack",
    )(lens, reflect, factor)


def unpacked(tile, start):
    row = lax.broadcasted_iota(jnp.int32, (KREF, BAND), 0)
    lane = lax.broadcasted_iota(jnp.int32, (KREF, BAND), 1)
    vectors = jnp.where(lane > row, tile, jnp.where(lane == row, 1.0, 0.0))
    vectors = pltpu.roll(vectors, start, 1)
    factor = jnp.where(lane <= row, tile, 0.0)[:, :KREF]
    scaled = product(halves(factor), halves(vectors))
    return [[jnp.where(part, v, 0.0) for part in (lane >= start, lane < start)] for v in (vectors, scaled)]


def apply_blocks(window, start, packed):
    ready = {j: unpacked(tile, start) for j, tile in packed.items()}
    tiles = {}
    for j in sorted({*packed, *(j + 1 for j in packed)}):
        parts = [(b, half) for half, b in enumerate((j, j - 1)) if b in packed]
        size = HALF if j not in packed else BAND
        tiles[j] = (parts, pl.ds(BAND * j, size), size)
    inner = {}
    for parts, place, size in tiles.values():
        left = jnp.concatenate([ready[b][0][half] for b, half in parts], axis=0)[:, :size]
        got = product(halves(left), halves(window[place, :]))
        for k, (b, _) in enumerate(parts):
            piece = got[k * KREF : (k + 1) * KREF]
            inner[b] = inner[b] + piece if b in inner else piece
    inner = {b: halves(value) for b, value in inner.items()}
    for parts, place, size in tiles.values():
        left = jnp.concatenate([ready[b][1][half] for b, half in parts], axis=0).T[:size]
        right = [jnp.concatenate([inner[b][k] for b, _ in parts], axis=0) for k in range(2)]
        window[place, :] = window[place, :] - product(halves(left), right)


def send_off(window, own, above, upward, downward):
    own[...] = window[ABOVE : ABOVE + ROWS, :]
    upward[...] = window[ABOVE : ABOVE + HALF, :]
    downward[:BAND, :] = window[ABOVE + ROWS - BAND : ABOVE + ROWS, :]
    step = KREF * BAND // COLS
    for k, tile in enumerate(above):
        for q in range(COLS // BAND):
            place = pl.ds(BAND + step * k, step)
            downward[place, q * BAND : (q + 1) * BAND] = tile[q * step : (q + 1) * step, :]


def received_tiles(message):
    step = KREF * BAND // COLS
    return [
        jnp.concatenate(
            [
                message[BAND + step * k : BAND + step * (k + 1), q * BAND : (q + 1) * BAND]
                for q in range(COLS // BAND)
            ],
            axis=0,
        )
        for k in range(2)
    ]


def first_kernel(starts, vectors, packed0, packed1, own, upward, downward, window):
    window[ABOVE : ABOVE + ROWS, :] = vectors[...]
    apply_blocks(window, starts[0], {b + 1: packed0[0, 0, b] for b in range(3)})
    send_off(window, own, [packed0[0, 0, 3], packed1[0, 0, 3]], upward, downward)


def join_pieces(window, vectors, from_above, from_below):
    window[:ABOVE, :] = from_above[:BAND, :]
    window[ABOVE : ABOVE + ROWS, :] = vectors[...]
    window[ABOVE + ROWS :, :] = from_below[...]


def middle_kernel(
    sweep, starts, vectors, from_above, from_below, pa, pb, pc, pd, own, upward, downward, window
):
    join_pieces(window, vectors, from_above, from_below)
    edge = received_tiles(from_above)
    apply_blocks(window, starts[sweep], {0: edge[0], 4: pa[0, 0, 3]})
    apply_blocks(
        window, starts[sweep + 1], {0: edge[1], **{b + 1: pb[0, 0, b] for b in range(4)}}
    )
    apply_blocks(window, starts[sweep + 2], {b + 1: pc[0, 0, b] for b in range(3)})
    send_off(window, own, [pc[0, 0, 3], pd[0, 0, 3]], upward, downward)


def last_kernel(
    sweep, starts, vectors, from_above, from_below, panel, pa, pb, own, partial, window
):
    join_pieces(window, vectors, from_above, from_below)
    edge = received_tiles(from_above)
    apply_blocks(window, starts[sweep], {0: edge[0], 4: pa[0, 0, 3]})
    apply_blocks(
        window, starts[sweep + 1], {0: edge[1], **{b + 1: pb[0, 0, b] for b in range(4)}}
    )
    done = window[ABOVE : ABOVE + ROWS, :]
    own[...] = done
    turned = panel[...].T
    partial[:, :COLS] = product(halves(turned), halves(done))
    partial[:, COLS:] = full_dot(turned, panel[...])


def whole(shape):
    return pl.BlockSpec(shape, lambda i: (0,) * len(shape))


def of_sweep(sweep):
    return pl.BlockSpec((1, 1, 4, KREF, BAND), lambda i: (sweep // 2, sweep % 2, 0, 0, 0))


OWN = (ROWS, COLS)
UP = (HALF, COLS)


def sent_shapes():
    return [jax.ShapeDtypeStruct(s, F32) for s in (OWN, UP, (DOWN, COLS))]


def call(kernel, out, in_specs, name):
    return pl.pallas_call(
        kernel,
        grid=(1,),
        out_shape=out,
        in_specs=in_specs,
        out_specs=[whole(o.shape) for o in out],
        scratch_shapes=[pltpu.VMEM((EXT, COLS), F32)],
        compiler_params=PARAMS,
        name=name,
    )


def first(starts, vectors, packed):
    specs = [SMEM, whole(OWN), of_sweep(0), of_sweep(1)]
    return call(first_kernel, sent_shapes(), specs, "first")(starts, vectors, packed, packed)


def middle(sweep, starts, vectors, from_above, from_below, packed):
    specs = [SMEM, whole(OWN), whole((DOWN, COLS)), whole(UP)]
    specs += [of_sweep(sweep + k) for k in range(4)]
    kernel = functools.partial(middle_kernel, sweep)
    run = call(kernel, sent_shapes(), specs, "middle")
    return run(starts, vectors, from_above, from_below, *[packed] * 4)


def last(sweep, starts, vectors, from_above, from_below, panel, packed):
    specs = [SMEM, whole(OWN), whole((DOWN, COLS)), whole(UP), whole((ROWS, BAND))]
    specs += [of_sweep(sweep + k) for k in range(2)]
    out = [jax.ShapeDtypeStruct(s, F32) for s in (OWN, (BAND, COLS + BAND))]
    kernel = functools.partial(last_kernel, sweep)
    run = call(kernel, out, specs, "last")
    return run(starts, vectors, from_above, from_below, panel, packed, packed)


def final_kernel(vectors, panel, total, out):
    row = lax.broadcasted_iota(jnp.int32, (BAND, BAND), 0)
    lane = lax.broadcasted_iota(jnp.int32, (BAND, BAND), 1)
    gram = total[:, COLS:]
    identity = jnp.where(row == lane, 1.0, 0.0)
    kept = 0.5 * gram * identity
    down = jnp.sum(kept, axis=1, keepdims=True)
    across = jnp.sum(kept, axis=0, keepdims=True)
    powered = jnp.where(lane > row, gram, 0.0) / down
    inverse = identity - powered
    reach = 1
    while reach * 2 < BAND:
        powered = full_dot(powered, powered)
        inverse = full_dot(inverse, identity + powered)
        reach = reach * 2
    inner = product(halves(inverse / across), halves(total[:, :COLS]))
    out[...] = vectors[...] - product(halves(panel[...]), halves(inner))


def final(vectors, panel, total):
    return pl.pallas_call(
        final_kernel,
        out_shape=jax.ShapeDtypeStruct(OWN, F32),
        in_specs=[VMEM] * 3,
        out_specs=VMEM,
        compiler_params=PARAMS,
        name="final",
    )(vectors, panel, total)


def shifted(value, steps):
    count = lax.axis_size("row")
    begin, end = max(0, -steps), min(count, count - steps)
    return lax.ppermute(value, "row", [(k, k + steps) for k in range(begin, end)])


def swapped(value, bit):
    return lax.ppermute(value, "row", [(k, k ^ bit) for k in range(lax.axis_size("row"))])


def spread(value, groups):
    return lax.all_to_all(
        value, "row", split_axis=0, concat_axis=0, tiled=True, axis_index_groups=groups
    )


def row_sum(value):
    count = lax.axis_size("row")
    groups = [list(range(k, count, 4)) for k in range(4)]
    size = count // 4
    core = lax.axis_index("row") % 2
    rows, width = value.shape
    half = rows // 2
    kept = lax.dynamic_slice_in_dim(value, core * half, half, 0)
    given = lax.dynamic_slice_in_dim(value, (1 - core) * half, half, 0)
    kept = kept + swapped(given, 1)
    share = spread(kept.reshape(size, half // size, width), groups).sum(axis=0)
    share = share + swapped(share, 2)
    copies = jnp.broadcast_to(share, (size, *share.shape))
    kept = spread(copies, groups).reshape(half, width)
    other = swapped(kept, 1)
    upper = jnp.where(core == 0, kept, other)
    lower = jnp.where(core == 0, other, kept)
    return jnp.concatenate([upper, lower], axis=0)


def body(sweep_start, block_len, reflectors, tfactors, panel, eigvecs):
    mine = reflectors.shape[0]
    col = lax.axis_index("col")
    lens = lax.dynamic_slice_in_dim(block_len, col * mine, mine, 0)
    packed = pack(lens, reflectors, tfactors)
    copies = jnp.broadcast_to(packed, (lax.axis_size("col"), *packed.shape))
    packed = lax.all_to_all(copies, "col", split_axis=0, concat_axis=0, tiled=True)
    sweeps = mine * lax.axis_size("col")
    vectors, upward, downward = first(sweep_start, eigvecs, packed)
    for sweep in range(0, sweeps, 2):
        from_below = shifted(upward, -1)
        from_above = shifted(downward, 1)
        pieces = (sweep_start, vectors, from_above, from_below)
        if sweep + 2 < sweeps:
            vectors, upward, downward = middle(sweep, *pieces, packed)
        else:
            vectors, partial = last(sweep, *pieces, panel, packed)
    return final(vectors, panel, row_sum(partial))


def solution(mesh):
    in_specs = (
        P(),
        P(None, "row"),
        P("col", "row", None, None),
        P("col", "row", None, None),
        P("row", None),
        P("row", "col"),
    )
    out_specs = P("row", "col")
    return jax.shard_map(body, mesh=mesh, in_specs=in_specs, out_specs=out_specs, check_vma=False)
```

```python
import functools

import jax
import jax.numpy as jnp
from jax import lax
from jax.experimental import pallas as pl
from jax.experimental.pallas import tpu as pltpu
from jax.sharding import PartitionSpec as P

F32 = jnp.float32
BF16 = jnp.bfloat16
BAND = 128
KREF = 64
HALF = 64
ROWS = 512
COLS = 512
ABOVE = BAND
EXT = ABOVE + ROWS + HALF
VMEM = pl.BlockSpec(memory_space=pltpu.VMEM)
SMEM = pl.BlockSpec(memory_space=pltpu.SMEM)
PARAMS = pltpu.CompilerParams(vmem_limit_bytes=20 * 1024 * 1024)


def halves(value):
    high = value.astype(BF16)
    return high, (value - high.astype(F32)).astype(BF16)


def product(left, right):
    (lh, ll), (rh, rl) = left, right
    dot = functools.partial(jnp.dot, preferred_element_type=F32)
    return dot(lh, rh) + (dot(ll, rh) + dot(lh, rl))


def full_dot(left, right):
    return jnp.dot(left, right, precision=lax.Precision.HIGHEST, preferred_element_type=F32)


def pack_kernel(lens, reflect, factor, out):
    row = lax.broadcasted_iota(jnp.int32, (KREF, BAND), 0)
    lane = lax.broadcasted_iota(jnp.int32, (KREF, BAND), 1)
    below = jnp.zeros((BAND - KREF, KREF), F32)
    for j in range(reflect.shape[0]):
        for b in range(reflect.shape[1]):
            side = jnp.concatenate([factor[j, b], below], axis=0)
            turned = jnp.concatenate([reflect[j, b], side], axis=1).T
            live = jnp.where(lane < lens[j, b], turned[:KREF], 0.0)
            out[j, b] = jnp.where(lane > row, live, turned[KREF:])


def pack(lens, reflect, factor):
    shape = (*reflect.shape[:2], KREF, BAND)
    return pl.pallas_call(
        pack_kernel,
        out_shape=jax.ShapeDtypeStruct(shape, F32),
        in_specs=[SMEM, VMEM, VMEM],
        out_specs=VMEM,
        compiler_params=PARAMS,
        name="pack",
    )(lens, reflect, factor)


def unpacked(tile, start, back):
    row = lax.broadcasted_iota(jnp.int32, (KREF, BAND), 0)
    lane = lax.broadcasted_iota(jnp.int32, (KREF, BAND), 1)
    vectors = jnp.where(lane > row, tile, jnp.where(lane == row, 1.0, 0.0))
    vectors = pltpu.roll(vectors, start, 1)
    factor = jnp.where(lane <= row, tile, 0.0)
    factor = factor.T[:KREF] if back else factor[:, :KREF]
    scaled = product(halves(factor), halves(vectors))
    return [[jnp.where(part, v, 0.0) for part in (lane >= start, lane < start)] for v in (vectors, scaled)]


def apply_blocks(window, start, packed, back=False):
    ready = {j: unpacked(tile, start, back) for j, tile in packed.items()}
    tiles = {}
    for j in sorted({*packed, *(j + 1 for j in packed)}):
        parts = [(b, half) for half, b in enumerate((j, j - 1)) if b in packed]
        size = HALF if j not in packed else BAND
        tiles[j] = (parts, pl.ds(BAND * j, size), size)
    inner = {}
    for parts, place, size in tiles.values():
        left = jnp.concatenate([ready[b][0][half] for b, half in parts], axis=0)[:, :size]
        got = product(halves(left), halves(window[place, :]))
        for k, (b, _) in enumerate(parts):
            piece = got[k * KREF : (k + 1) * KREF]
            inner[b] = inner[b] + piece if b in inner else piece
    inner = {b: halves(value) for b, value in inner.items()}
    for parts, place, size in tiles.values():
        left = jnp.concatenate([ready[b][1][half] for b, half in parts], axis=0).T[:size]
        right = [jnp.concatenate([inner[b][k] for b, _ in parts], axis=0) for k in range(2)]
        window[place, :] = window[place, :] - product(halves(left), right)


def slabs(width, tiles):
    across = width // BAND
    for n in range(tiles * KREF // 8):
        yield n // (KREF // 8), n % (KREF // 8) * 8, BAND + n // across * 8, n % across * BAND


def message_rows(width, tiles):
    return BAND + -(-tiles * KREF // 8 // (width // BAND)) * 8


def send_off(windows, upward, downward, tiles):
    left = 0
    for window in windows:
        columns = pl.ds(left, window.shape[1])
        upward[:, columns] = window[ABOVE : ABOVE + HALF, :]
        downward[:BAND, columns] = window[ABOVE + ROWS - BAND : ABOVE + ROWS, :]
        left += window.shape[1]
    for k, low, row, lane in slabs(left, len(tiles)):
        downward[row : row + 8, lane : lane + BAND] = tiles[k][low : low + 8, :]


def join_pieces(windows, owns, from_above, from_below):
    left = 0
    for window, own in zip(windows, owns):
        columns = pl.ds(left, window.shape[1])
        window[:ABOVE, :] = from_above[:BAND, columns]
        window[ABOVE : ABOVE + ROWS, :] = own[...]
        window[ABOVE + ROWS :, :] = from_below[:, columns]
        left += window.shape[1]
    tiles = [[] for _ in range(2 * len(windows))]
    for k, _, row, lane in slabs(left, len(tiles)):
        tiles[k].append(from_above[row : row + 8, lane : lane + BAND])
    return [jnp.concatenate(parts, axis=0) for parts in tiles]


def inner(packed):
    return {b + 1: packed[0, 0, b] for b in range(3)}


def outer(above, packed):
    return {0: above, 4: packed[0, 0, 3]}


def every(above, packed):
    return {0: above, **{b + 1: packed[0, 0, b] for b in range(4)}}


def two_sweeps(window, starts, sweeps, edge, packed, back=False):
    apply_blocks(window, starts[sweeps[0]], outer(edge[0], packed[0]), back)
    apply_blocks(window, starts[sweeps[1]], every(edge[1], packed[1]), back)


def first_kernel(
    last_sweep, starts, vectors, panel, p0, p1, q0, q1, own, reduced, upward, downward, wide, narrow
):
    wide[ABOVE : ABOVE + ROWS, :] = vectors[...]
    narrow[ABOVE : ABOVE + ROWS, :] = panel[...]
    apply_blocks(wide, starts[0], inner(p0))
    apply_blocks(narrow, starts[last_sweep], inner(q0), True)
    send_off((wide, narrow), upward, downward, [p[0, 0, 3] for p in (p0, p1, q0, q1)])
    own[...] = wide[ABOVE : ABOVE + ROWS, :]
    reduced[...] = narrow[ABOVE : ABOVE + ROWS, :]


def second_kernel(
    last_sweep, starts, vectors, panel, above, below, p0, p1, p2, p3, q0, q1, q2, q3,
    own, reduced, upward, downward, wide, narrow,
):
    edge = join_pieces((wide, narrow), (vectors, panel), above, below)
    two_sweeps(wide, starts, (0, 1), edge[:2], (p0, p1))
    two_sweeps(narrow, starts, (last_sweep, last_sweep - 1), edge[2:], (q0, q1), True)
    apply_blocks(wide, starts[2], inner(p2))
    apply_blocks(narrow, starts[last_sweep - 2], inner(q2), True)
    send_off((wide, narrow), upward, downward, [p[0, 0, 3] for p in (p2, p3, q2, q3)])
    own[...] = wide[ABOVE : ABOVE + ROWS, :]
    reduced[...] = narrow[ABOVE : ABOVE + ROWS, :]


def third_kernel(
    last_sweep, starts, vectors, panel, above, below, p0, p1, p2, p3, q0, q1,
    own, between, reduced, upward, downward, wide, narrow,
):
    edge = join_pieces((wide, narrow), (vectors, panel), above, below)
    two_sweeps(wide, starts, (2, 3), edge[:2], (p0, p1))
    two_sweeps(narrow, starts, (last_sweep - 2, last_sweep - 3), edge[2:], (q0, q1), True)
    between[...] = wide[ABOVE : ABOVE + ROWS, :]
    reduced[...] = narrow[ABOVE : ABOVE + ROWS, :]
    apply_blocks(wide, starts[4], inner(p2))
    send_off((wide,), upward, downward, [p[0, 0, 3] for p in (p2, p3)])
    own[...] = wide[ABOVE : ABOVE + ROWS, :]


def middle_kernel(
    sweep, starts, vectors, above, below, p0, p1, p2, p3, own, upward, downward, wide
):
    edge = join_pieces((wide,), (vectors,), above, below)
    two_sweeps(wide, starts, (sweep, sweep + 1), edge, (p0, p1))
    apply_blocks(wide, starts[sweep + 2], inner(p2))
    send_off((wide,), upward, downward, [p[0, 0, 3] for p in (p2, p3)])
    own[...] = wide[ABOVE : ABOVE + ROWS, :]


def last_kernel(sweep, starts, vectors, above, below, p0, p1, own, wide):
    edge = join_pieces((wide,), (vectors,), above, below)
    two_sweeps(wide, starts, (sweep, sweep + 1), edge, (p0, p1))
    own[...] = wide[ABOVE : ABOVE + ROWS, :]


def project_kernel(panel, reduced, vectors, partial):
    partial[:, :COLS] = product(halves(reduced[...].T), halves(vectors[...]))
    partial[:, COLS:] = full_dot(panel[...].T, panel[...])


def whole(shape):
    return pl.BlockSpec(shape, lambda i: (0,) * len(shape))


def of_sweep(sweep):
    return pl.BlockSpec((1, 1, 4, KREF, BAND), lambda i: (sweep // 2, sweep % 2, 0, 0, 0))


OWN = (ROWS, COLS)
THIN = (ROWS, BAND)


def sent(width, tiles):
    return [(HALF, width), (message_rows(width, tiles), width)]


def call(kernel, out, operands, packed, sweeps, widths):
    specs = [SMEM] + [whole(o.shape) for o in operands[1:]] + [of_sweep(s) for s in sweeps]
    run = pl.pallas_call(
        kernel,
        grid=(1,),
        out_shape=[jax.ShapeDtypeStruct(s, F32) for s in out],
        in_specs=specs,
        out_specs=[whole(s) for s in out],
        scratch_shapes=[pltpu.VMEM((EXT, w), F32) for w in widths],
        compiler_params=PARAMS,
    )
    return run(*operands, *[packed] * len(sweeps))


def project(panel, reduced, vectors):
    return pl.pallas_call(
        project_kernel,
        out_shape=jax.ShapeDtypeStruct((BAND, COLS + BAND), F32),
        in_specs=[VMEM] * 3,
        out_specs=VMEM,
        compiler_params=PARAMS,
        name="project",
    )(panel, reduced, vectors)


def final_kernel(vectors, panel, total, out):
    row = lax.broadcasted_iota(jnp.int32, (BAND, BAND), 0)
    lane = lax.broadcasted_iota(jnp.int32, (BAND, BAND), 1)
    gram = total[:, COLS:]
    identity = jnp.where(row == lane, 1.0, 0.0)
    kept = 0.5 * gram * identity
    down = jnp.sum(kept, axis=1, keepdims=True)
    across = jnp.sum(kept, axis=0, keepdims=True)
    powered = jnp.where(lane > row, gram, 0.0) / down
    inverse = identity - powered
    reach = 1
    while reach * 2 < BAND:
        powered = full_dot(powered, powered)
        inverse = full_dot(inverse, identity + powered)
        reach = reach * 2
    inner = product(halves(inverse / across), halves(total[:, :COLS]))
    out[...] = vectors[...] - product(halves(panel[...]), halves(inner))


def final(vectors, panel, total):
    return pl.pallas_call(
        final_kernel,
        out_shape=jax.ShapeDtypeStruct(OWN, F32),
        in_specs=[VMEM] * 3,
        out_specs=VMEM,
        compiler_params=PARAMS,
        name="final",
    )(vectors, panel, total)


def shifted(value, steps):
    count = lax.axis_size("row")
    begin, end = max(0, -steps), min(count, count - steps)
    return lax.ppermute(value, "row", [(k, k + steps) for k in range(begin, end)])


def swapped(value, bit):
    return lax.ppermute(value, "row", [(k, k ^ bit) for k in range(lax.axis_size("row"))])


def spread(value, groups):
    return lax.all_to_all(
        value, "row", split_axis=0, concat_axis=0, tiled=True, axis_index_groups=groups
    )


def row_sum(value):
    count = lax.axis_size("row")
    groups = [list(range(k, count, 4)) for k in range(4)]
    size = count // 4
    core = lax.axis_index("row") % 2
    rows, width = value.shape
    half = rows // 2
    kept = lax.dynamic_slice_in_dim(value, core * half, half, 0)
    given = lax.dynamic_slice_in_dim(value, (1 - core) * half, half, 0)
    kept = kept + swapped(given, 1)
    share = spread(kept.reshape(size, half // size, width), groups).sum(axis=0)
    share = share + swapped(share, 2)
    copies = jnp.broadcast_to(share, (size, *share.shape))
    kept = spread(copies, groups).reshape(half, width)
    other = swapped(kept, 1)
    upper = jnp.where(core == 0, kept, other)
    lower = jnp.where(core == 0, other, kept)
    return jnp.concatenate([upper, lower], axis=0)


def body(sweep_start, block_len, reflectors, tfactors, panel, eigvecs):
    mine = reflectors.shape[0]
    col = lax.axis_index("col")
    lens = lax.dynamic_slice_in_dim(block_len, col * mine, mine, 0)
    packed = pack(lens, reflectors, tfactors)
    copies = jnp.broadcast_to(packed, (lax.axis_size("col"), *packed.shape))
    packed = lax.all_to_all(copies, "col", split_axis=0, concat_axis=0, tiled=True)
    end = mine * lax.axis_size("col") - 1
    both = (COLS, BAND)
    wide = COLS + BAND

    def exchanged(upward, downward):
        above = shifted(downward, 1)
        return above, shifted(upward, -1)

    vectors, reduced, upward, downward = call(
        functools.partial(first_kernel, end), [OWN, THIN, *sent(wide, 4)],
        (sweep_start, eigvecs, panel), packed, (0, 1, end, end - 1), both,
    )
    vectors, reduced, upward, downward = call(
        functools.partial(second_kernel, end), [OWN, THIN, *sent(wide, 4)],
        (sweep_start, vectors, reduced, *exchanged(upward, downward)), packed,
        (0, 1, 2, 3, end, end - 1, end - 2, end - 3), both,
    )
    vectors, between, reduced, upward, downward = call(
        functools.partial(third_kernel, end), [OWN, OWN, THIN, *sent(COLS, 2)],
        (sweep_start, vectors, reduced, *exchanged(upward, downward)), packed,
        (2, 3, 4, 5, end - 2, end - 3), both,
    )
    total = row_sum(project(panel, reduced, between))
    vectors, upward, downward = call(
        functools.partial(middle_kernel, 4), [OWN, *sent(COLS, 2)],
        (sweep_start, vectors, *exchanged(upward, downward)), packed, (4, 5, 6, 7), (COLS,),
    )
    (vectors,) = call(
        functools.partial(last_kernel, 6), [OWN],
        (sweep_start, vectors, *exchanged(upward, downward)), packed, (6, 7), (COLS,),
    )
    return final(vectors, panel, total)


def solution(mesh):
    in_specs = (
        P(),
        P(None, "row"),
        P("col", "row", None, None),
        P("col", "row", None, None),
        P("row", None),
        P("row", "col"),
    )
    out_specs = P("row", "col")
    return jax.shard_map(body, mesh=mesh, in_specs=in_specs, out_specs=out_specs, check_vma=False)
```

```python
import functools

import jax
import jax.numpy as jnp
from jax import lax
from jax.experimental import pallas as pl
from jax.experimental.pallas import tpu as pltpu
from jax.sharding import PartitionSpec as P

F32 = jnp.float32
BF16 = jnp.bfloat16
BAND = 128
KREF = 64
HALF = 64
ROWS = 512
COLS = 512
ABOVE = BAND
EXT = ABOVE + ROWS + HALF
EXTRA = 2 * KREF * BAND // COLS
DOWN = BAND + EXTRA
VMEM = pl.BlockSpec(memory_space=pltpu.VMEM)
SMEM = pl.BlockSpec(memory_space=pltpu.SMEM)
PARAMS = pltpu.CompilerParams(vmem_limit_bytes=24 * 1024 * 1024)


def halves(value):
    high = value.astype(BF16)
    return high, (value - high.astype(F32)).astype(BF16)


def product(left, right):
    (lh, ll), (rh, rl) = left, right
    dot = functools.partial(jnp.dot, preferred_element_type=F32)
    return dot(lh, rh) + (dot(ll, rh) + dot(lh, rl))


def full_dot(left, right):
    return jnp.dot(left, right, precision=lax.Precision.HIGHEST, preferred_element_type=F32)


def pack_kernel(lens, reflect, factor, out):
    row = lax.broadcasted_iota(jnp.int32, (KREF, BAND), 0)
    lane = lax.broadcasted_iota(jnp.int32, (KREF, BAND), 1)
    below = jnp.zeros((BAND - KREF, KREF), F32)
    for j in range(reflect.shape[0]):
        for b in range(reflect.shape[1]):
            side = jnp.concatenate([factor[j, b], below], axis=0)
            turned = jnp.concatenate([reflect[j, b], side], axis=1).T
            live = jnp.where(lane < lens[j, b], turned[:KREF], 0.0)
            out[j, b] = jnp.where(lane > row, live, turned[KREF:])


def pack(lens, reflect, factor):
    shape = (*reflect.shape[:2], KREF, BAND)
    return pl.pallas_call(
        pack_kernel,
        out_shape=jax.ShapeDtypeStruct(shape, F32),
        in_specs=[SMEM, VMEM, VMEM],
        out_specs=VMEM,
        compiler_params=PARAMS,
        name="pack",
    )(lens, reflect, factor)


def unpacked(tile, start):
    row = lax.broadcasted_iota(jnp.int32, (KREF, BAND), 0)
    lane = lax.broadcasted_iota(jnp.int32, (KREF, BAND), 1)
    vectors = jnp.where(lane > row, tile, jnp.where(lane == row, 1.0, 0.0))
    vectors = pltpu.roll(vectors, start, 1)
    factor = jnp.where(lane <= row, tile, 0.0)[:, :KREF]
    scaled = product(halves(factor), halves(vectors))
    return [[jnp.where(part, v, 0.0) for part in (lane >= start, lane < start)] for v in (vectors, scaled)]


def apply_blocks(tiles, start, packed):
    ready = {j: unpacked(tile, start) for j, tile in packed.items()}
    work = {}
    for j in sorted({*packed, *(j + 1 for j in packed)}):
        parts = [(b, half) for half, b in enumerate((j, j - 1)) if b in packed]
        size = HALF if j not in packed else BAND
        ref, first = tiles[j]
        work[j] = (parts, ref, pl.ds(first, size), size)
    inner = {}
    for parts, ref, place, size in work.values():
        left = jnp.concatenate([ready[b][0][half] for b, half in parts], axis=0)[:, :size]
        got = product(halves(left), halves(ref[place, :]))
        for k, (b, _) in enumerate(parts):
            piece = got[k * KREF : (k + 1) * KREF]
            inner[b] = inner[b] + piece if b in inner else piece
    inner = {b: halves(value) for b, value in inner.items()}
    for parts, ref, place, size in work.values():
        left = jnp.concatenate([ready[b][1][half] for b, half in parts], axis=0).T[:size]
        right = [jnp.concatenate([inner[b][k] for b, _ in parts], axis=0) for k in range(2)]
        ref[place, :] = ref[place, :] - product(halves(left), right)


def tiles_of(own, above=None, below=None):
    tiles = {j + 1: (own, BAND * j) for j in range(ROWS // BAND)}
    tiles[0] = (above, 0)
    tiles[ROWS // BAND + 1] = (below, 0)
    return tiles


def block(packed, sweep, b):
    return packed[sweep // 2, sweep % 2, b]


def send_down(own, message, packed, sweep):
    message[:BAND, :] = own[ROWS - BAND :, :]
    step = KREF * BAND // COLS
    for k in range(2):
        tile = block(packed, sweep + k, 3)
        for q in range(COLS // BAND):
            place = pl.ds(BAND + step * k, step)
            message[place, q * BAND : (q + 1) * BAND] = tile[q * step : (q + 1) * step, :]


def received_tile(message, k):
    step = KREF * BAND // COLS
    rows = pl.ds(BAND + step * k, step)
    parts = [message[rows, q * BAND : (q + 1) * BAND] for q in range(COLS // BAND)]
    return jnp.concatenate(parts, axis=0)


def first_lower(starts, packed, _, own, message):
    apply_blocks(tiles_of(own), starts[0], {3: block(packed, 0, 2)})
    send_down(own, message, packed, 0)


def first_upper(starts, packed, _, own, message):
    apply_blocks(tiles_of(own), starts[0], {j: block(packed, 0, j - 1) for j in (1, 2)})
    message[...] = own[:HALF, :]


def lower(sweep, starts, packed, _, received, own, *rest):
    below = rest[-1]
    below[...] = received[...]
    tiles = tiles_of(own, below=below)
    apply_blocks(tiles, starts[sweep], {4: block(packed, sweep, 3)})
    apply_blocks(tiles, starts[sweep + 1], {j: block(packed, sweep + 1, j - 1) for j in (2, 3, 4)})
    if len(rest) > 1:
        apply_blocks(tiles, starts[sweep + 2], {3: block(packed, sweep + 2, 2)})
        send_down(own, rest[0], packed, sweep + 2)


def upper(sweep, starts, packed, _, received, own, *rest):
    above = rest[-1]
    above[...] = received[:BAND, :]
    tiles = tiles_of(own, above=above)
    apply_blocks(tiles, starts[sweep], {0: received_tile(received, 0)})
    second = {0: received_tile(received, 1), 1: block(packed, sweep + 1, 0)}
    apply_blocks(tiles, starts[sweep + 1], second)
    if len(rest) > 1:
        third = {j: block(packed, sweep + 2, j - 1) for j in (1, 2)}
        apply_blocks(tiles, starts[sweep + 2], third)
        rest[0][...] = own[:HALF, :]


OWN = (ROWS, COLS)
UP = (HALF, COLS)
DOWN = (BAND + 2 * KREF * BAND // COLS, COLS)


def step(kernel, name, message, scratch, starts, packed, vectors, *received):
    out = [OWN] + ([message] if message else [])
    return pl.pallas_call(
        kernel,
        out_shape=[jax.ShapeDtypeStruct(s, F32) for s in out],
        in_specs=[SMEM] + [VMEM] * (2 + len(received)),
        out_specs=[VMEM] * len(out),
        scratch_shapes=[pltpu.VMEM(s, F32) for s in scratch],
        input_output_aliases={2: 0},
        compiler_params=PARAMS,
        name=name,
    )(starts, packed, vectors, *received)


def project_kernel(panel, vectors, partial):
    turned = panel[...].T
    partial[:, :COLS] = product(halves(turned), halves(vectors[...]))
    partial[:, COLS:] = full_dot(turned, panel[...])


def project(panel, vectors):
    return pl.pallas_call(
        project_kernel,
        out_shape=jax.ShapeDtypeStruct((BAND, COLS + BAND), F32),
        in_specs=[VMEM] * 2,
        out_specs=VMEM,
        compiler_params=PARAMS,
        name="project",
    )(panel, vectors)


def final_kernel(vectors, panel, total, out):
    row = lax.broadcasted_iota(jnp.int32, (BAND, BAND), 0)
    lane = lax.broadcasted_iota(jnp.int32, (BAND, BAND), 1)
    gram = total[:, COLS:]
    identity = jnp.where(row == lane, 1.0, 0.0)
    kept = 0.5 * gram * identity
    down = jnp.sum(kept, axis=1, keepdims=True)
    across = jnp.sum(kept, axis=0, keepdims=True)
    powered = jnp.where(lane > row, gram, 0.0) / down
    inverse = identity - powered
    reach = 1
    while reach * 2 < BAND:
        powered = full_dot(powered, powered)
        inverse = full_dot(inverse, identity + powered)
        reach = reach * 2
    inner = product(halves(inverse / across), halves(total[:, :COLS]))
    out[...] = vectors[...] - product(halves(panel[...]), halves(inner))


def final(vectors, panel, total):
    return pl.pallas_call(
        final_kernel,
        out_shape=jax.ShapeDtypeStruct(OWN, F32),
        in_specs=[VMEM] * 3,
        out_specs=VMEM,
        compiler_params=PARAMS,
        name="final",
    )(vectors, panel, total)


def shifted(value, steps):
    count = lax.axis_size("row")
    begin, end = max(0, -steps), min(count, count - steps)
    return lax.ppermute(value, "row", [(k, k + steps) for k in range(begin, end)])


def swapped(value, bit):
    return lax.ppermute(value, "row", [(k, k ^ bit) for k in range(lax.axis_size("row"))])


def spread(value, groups):
    return lax.all_to_all(
        value, "row", split_axis=0, concat_axis=0, tiled=True, axis_index_groups=groups
    )


def row_sum(value):
    count = lax.axis_size("row")
    groups = [list(range(k, count, 4)) for k in range(4)]
    size = count // 4
    core = lax.axis_index("row") % 2
    rows, width = value.shape
    half = rows // 2
    kept = lax.dynamic_slice_in_dim(value, core * half, half, 0)
    given = lax.dynamic_slice_in_dim(value, (1 - core) * half, half, 0)
    kept = kept + swapped(given, 1)
    share = spread(kept.reshape(size, half // size, width), groups).sum(axis=0)
    share = share + swapped(share, 2)
    copies = jnp.broadcast_to(share, (size, *share.shape))
    kept = spread(copies, groups).reshape(half, width)
    other = swapped(kept, 1)
    upper = jnp.where(core == 0, kept, other)
    lower = jnp.where(core == 0, other, kept)
    return jnp.concatenate([upper, lower], axis=0)


def body(sweep_start, block_len, reflectors, tfactors, panel, eigvecs):
    mine = reflectors.shape[0]
    col = lax.axis_index("col")
    lens = lax.dynamic_slice_in_dim(block_len, col * mine, mine, 0)
    packed = pack(lens, reflectors, tfactors)
    copies = jnp.broadcast_to(packed, (lax.axis_size("col"), *packed.shape))
    packed = lax.all_to_all(copies, "col", split_axis=0, concat_axis=0, tiled=True)
    sweeps = mine * lax.axis_size("col")
    fixed = (sweep_start, packed)
    vectors, downward = step(first_lower, "first_lower", DOWN, (), *fixed, eigvecs)
    from_above = shifted(downward, 1)
    vectors, upward = step(first_upper, "first_upper", UP, (), *fixed, vectors)
    from_below = shifted(upward, -1)
    for sweep in range(0, sweeps - 2, 2):
        kernel = functools.partial(lower, sweep)
        vectors, downward = step(kernel, "lower", DOWN, (UP,), *fixed, vectors, from_below)
        later = shifted(downward, 1)
        kernel = functools.partial(upper, sweep)
        above = (BAND, COLS)
        vectors, upward = step(kernel, "upper", UP, (above,), *fixed, vectors, from_above)
        from_below = shifted(upward, -1)
        from_above = later
    kernel = functools.partial(lower, sweeps - 2)
    (vectors,) = step(kernel, "last_lower", None, (UP,), *fixed, vectors, from_below)
    kernel = functools.partial(upper, sweeps - 2)
    (vectors,) = step(kernel, "last_upper", None, ((BAND, COLS),), *fixed, vectors, from_above)
    return final(vectors, panel, row_sum(project(panel, vectors)))


def solution(mesh):
    in_specs = (
        P(),
        P(None, "row"),
        P("col", "row", None, None),
        P("col", "row", None, None),
        P("row", None),
        P("row", "col"),
    )
    out_specs = P("row", "col")
    return jax.shard_map(body, mesh=mesh, in_specs=in_specs, out_specs=out_specs, check_vma=False)
```

```python
import functools

import jax
import jax.numpy as jnp
from jax import lax
from jax.experimental import pallas as pl
from jax.experimental.pallas import tpu as pltpu
from jax.sharding import PartitionSpec as P

F32 = jnp.float32
BF16 = jnp.bfloat16
BAND = 128
KREF = 64
HALF = 64
ROWS = 512
COLS = 512
VMEM = pl.BlockSpec(memory_space=pltpu.VMEM)
SMEM = pl.BlockSpec(memory_space=pltpu.SMEM)
PARAMS = pltpu.CompilerParams(vmem_limit_bytes=24 * 1024 * 1024)


def halves(value):
    high = value.astype(BF16)
    return high, (value - high.astype(F32)).astype(BF16)


def product(left, right):
    (lh, ll), (rh, rl) = left, right
    dot = functools.partial(jnp.dot, preferred_element_type=F32)
    return dot(jnp.concatenate([lh, ll, lh], axis=1), jnp.concatenate([rh, rh, rl], axis=0))


def full_dot(left, right):
    return jnp.dot(left, right, precision=lax.Precision.HIGHEST, preferred_element_type=F32)


def pack_kernel(lens, reflect, factor, out):
    row = lax.broadcasted_iota(jnp.int32, (KREF, BAND), 0)
    lane = lax.broadcasted_iota(jnp.int32, (KREF, BAND), 1)
    below = jnp.zeros((BAND - KREF, KREF), F32)
    for j in range(reflect.shape[0]):
        for b in range(reflect.shape[1]):
            side = jnp.concatenate([factor[j, b], below], axis=0)
            turned = jnp.concatenate([reflect[j, b], side], axis=1).T
            live = jnp.where(lane < lens[j, b], turned[:KREF], 0.0)
            out[j, b] = jnp.where(lane > row, live, turned[KREF:])


def pack(lens, reflect, factor):
    shape = (*reflect.shape[:2], KREF, BAND)
    return pl.pallas_call(
        pack_kernel,
        out_shape=jax.ShapeDtypeStruct(shape, F32),
        in_specs=[SMEM, VMEM, VMEM],
        out_specs=VMEM,
        compiler_params=PARAMS,
        name="pack",
    )(lens, reflect, factor)


def unpacked(tile, start):
    row = lax.broadcasted_iota(jnp.int32, (KREF, BAND), 0)
    lane = lax.broadcasted_iota(jnp.int32, (KREF, BAND), 1)
    vectors = jnp.where(lane > row, tile, jnp.where(lane == row, 1.0, 0.0))
    vectors = pltpu.roll(vectors, start, 1)
    factor = jnp.where(lane <= row, tile, 0.0)[:, :KREF]
    scaled = product(halves(factor), halves(vectors))
    return [[jnp.where(part, v, 0.0) for part in (lane >= start, lane < start)] for v in (vectors, scaled)]


def plan(blocks):
    work = []
    for j in sorted({*blocks, *(j + 1 for j in blocks)}):
        parts = [(b, half) for half, b in enumerate((j, j - 1)) if b in blocks]
        work.append((j, parts, BAND if j in blocks else HALF))
    return work


def tripled(left):
    high, low = halves(left)
    return jnp.concatenate([high, low, high], axis=1)


def prepare_kernel(groups, starts, packed, *rest):
    front, back = rest[-2:]
    n = 0
    for sweep, blocks in groups:
        ready = {}
        for j, b in blocks.items():
            tile = packed[sweep // 2, sweep % 2, b] if j > 0 else received_tile(rest[0], b)
            ready[j] = unpacked(tile, starts[sweep])
        for _, parts, size in plan(blocks):
            span = KREF * len(parts)
            left = jnp.concatenate([ready[b][0][half] for b, half in parts], axis=0)
            front[n, :span, : 3 * size] = tripled(left[:, :size])
            left = jnp.concatenate([ready[b][1][half] for b, half in parts], axis=0).T
            back[n, :size, : 3 * span] = tripled(left[:size])
            n += 1


def prepare(groups, *operands):
    count = sum(len(plan(blocks)) for _, blocks in groups)
    shape = jax.ShapeDtypeStruct((count, BAND, 3 * BAND), BF16)
    return pl.pallas_call(
        functools.partial(prepare_kernel, groups),
        out_shape=[shape] * 2,
        in_specs=[SMEM] + [VMEM] * (len(operands) - 1),
        out_specs=[VMEM] * 2,
        compiler_params=PARAMS,
        name="prepare",
    )(*operands)


def stacked(value):
    high, low = halves(value)
    return jnp.concatenate([high, high, low], axis=0)


def apply_groups(tiles, groups, front, back):
    n = 0
    for _, blocks in groups:
        work = plan(blocks)
        inner = {}
        for k, (j, parts, size) in enumerate(work):
            ref, first = tiles[j]
            left = front[n + k, : KREF * len(parts), : 3 * size]
            right = stacked(ref[pl.ds(first, size), :])
            got = jnp.dot(left, right, preferred_element_type=F32)
            for m, (b, _) in enumerate(parts):
                piece = got[m * KREF : (m + 1) * KREF]
                inner[b] = inner[b] + piece if b in inner else piece
        for k, (j, parts, size) in enumerate(work):
            ref, first = tiles[j]
            left = back[n + k, :size, : 3 * KREF * len(parts)]
            right = stacked(jnp.concatenate([inner[b] for b, _ in parts], axis=0))
            place = pl.ds(first, size)
            ref[place, :] = ref[place, :] - jnp.dot(left, right, preferred_element_type=F32)
        n += len(work)


def tiles_of(own, above=None, below=None):
    tiles = {j + 1: (own, BAND * j) for j in range(ROWS // BAND)}
    tiles[0] = (above, 0)
    tiles[ROWS // BAND + 1] = (below, 0)
    return tiles


def down_rows(count):
    return BAND + count * KREF * BAND // COLS


def send_down(own, message, packed, sweeps):
    message[:BAND, :] = own[ROWS - BAND :, :]
    step = KREF * BAND // COLS
    for k, sweep in enumerate(sweeps):
        tile = packed[sweep // 2, sweep % 2, 3]
        for q in range(COLS // BAND):
            place = pl.ds(BAND + step * k, step)
            message[place, q * BAND : (q + 1) * BAND] = tile[q * step : (q + 1) * step, :]


def received_tile(message, k):
    step = KREF * BAND // COLS
    rows = pl.ds(BAND + step * k, step)
    parts = [message[rows, q * BAND : (q + 1) * BAND] for q in range(COLS // BAND)]
    return jnp.concatenate(parts, axis=0)


def lower(groups, sent, fresh, vectors, front, back, packed, *rest):
    rest = list(rest)
    received = None if fresh else rest.pop(0)
    own = rest.pop(0)
    message = None if sent is None else rest.pop(0)
    below = None if fresh else rest.pop(0)
    if fresh:
        own[...] = vectors[...]
    else:
        below[...] = received[...]
    apply_groups(tiles_of(own, below=below), groups, front, back)
    if sent is not None:
        send_down(own, message, packed, sent)


def upper(groups, send, fresh, vectors, front, back, *rest):
    rest = list(rest)
    received = None if fresh else rest.pop(0)
    own = rest.pop(0)
    message = rest.pop(0) if send else None
    above = None if fresh else rest.pop(0)
    if not fresh:
        above[...] = received[:BAND, :]
    apply_groups(tiles_of(own, above=above), groups, front, back)
    if send:
        message[...] = own[:HALF, :]


OWN = (ROWS, COLS)
UP = (HALF, COLS)


def step(kernel, message, scratch, alias, *operands):
    out = [OWN] + ([message] if message else [])
    return pl.pallas_call(
        kernel,
        out_shape=[jax.ShapeDtypeStruct(s, F32) for s in out],
        in_specs=[VMEM] * len(operands),
        out_specs=[VMEM] * len(out),
        scratch_shapes=[pltpu.VMEM(s, F32) for s in scratch],
        input_output_aliases={0: 0} if alias else {},
        compiler_params=PARAMS,
    )(*operands)


def project_kernel(panel, vectors, partial):
    turned = panel[...].T
    partial[:, :COLS] = product(halves(turned), halves(vectors[...]))
    partial[:, COLS:] = full_dot(turned, panel[...])


def project(panel, vectors):
    return pl.pallas_call(
        project_kernel,
        out_shape=jax.ShapeDtypeStruct((BAND, COLS + BAND), F32),
        in_specs=[VMEM] * 2,
        out_specs=VMEM,
        compiler_params=PARAMS,
        name="project",
    )(panel, vectors)


def final_kernel(vectors, panel, total, out):
    row = lax.broadcasted_iota(jnp.int32, (BAND, BAND), 0)
    lane = lax.broadcasted_iota(jnp.int32, (BAND, BAND), 1)
    gram = total[:, COLS:]
    identity = jnp.where(row == lane, 1.0, 0.0)
    kept = 0.5 * gram * identity
    down = jnp.sum(kept, axis=1, keepdims=True)
    across = jnp.sum(kept, axis=0, keepdims=True)
    powered = jnp.where(lane > row, gram, 0.0) / down
    inverse = identity - powered
    reach = 1
    while reach * 2 < BAND:
        powered = full_dot(powered, powered)
        inverse = full_dot(inverse, identity + powered)
        reach = reach * 2
    inner = product(halves(inverse / across), halves(total[:, :COLS]))
    out[...] = vectors[...] - product(halves(panel[...]), halves(inner))


def final(vectors, panel, total):
    return pl.pallas_call(
        final_kernel,
        out_shape=jax.ShapeDtypeStruct(OWN, F32),
        in_specs=[VMEM] * 3,
        out_specs=VMEM,
        compiler_params=PARAMS,
        name="final",
    )(vectors, panel, total)


def shifted(value, steps):
    count = lax.axis_size("row")
    begin, end = max(0, -steps), min(count, count - steps)
    return lax.ppermute(value, "row", [(k, k + steps) for k in range(begin, end)])


def swapped(value, bit):
    return lax.ppermute(value, "row", [(k, k ^ bit) for k in range(lax.axis_size("row"))])


def spread(value, groups):
    return lax.all_to_all(
        value, "row", split_axis=0, concat_axis=0, tiled=True, axis_index_groups=groups
    )


def row_sum(value):
    count = lax.axis_size("row")
    groups = [list(range(k, count, 4)) for k in range(4)]
    size = count // 4
    core = lax.axis_index("row") % 2
    rows, width = value.shape
    half = rows // 2
    kept = lax.dynamic_slice_in_dim(value, core * half, half, 0)
    given = lax.dynamic_slice_in_dim(value, (1 - core) * half, half, 0)
    kept = kept + swapped(given, 1)
    share = spread(kept.reshape(size, half // size, width), groups).sum(axis=0)
    share = share + swapped(share, 2)
    copies = jnp.broadcast_to(share, (size, *share.shape))
    kept = spread(copies, groups).reshape(half, width)
    other = swapped(kept, 1)
    upper = jnp.where(core == 0, kept, other)
    lower = jnp.where(core == 0, other, kept)
    return jnp.concatenate([upper, lower], axis=0)


def body(sweep_start, block_len, reflectors, tfactors, panel, eigvecs):
    mine = reflectors.shape[0]
    col = lax.axis_index("col")
    lens = lax.dynamic_slice_in_dim(block_len, col * mine, mine, 0)
    packed = pack(lens, reflectors, tfactors)
    copies = jnp.broadcast_to(packed, (lax.axis_size("col"), *packed.shape))
    packed = lax.all_to_all(copies, "col", split_axis=0, concat_axis=0, tiled=True)
    sweeps = mine * lax.axis_size("col")
    fixed = (sweep_start, packed)
    low = [(0, {3: 2})]
    high = [(0, {1: 0, 2: 1})]
    ahead = 4
    ready = prepare(low, *fixed)
    also = prepare(high, *fixed)
    kernel = functools.partial(lower, low, range(ahead), True)
    message = (down_rows(ahead), COLS)
    vectors, downward = step(kernel, message, (), False, eigvecs, *ready, packed)
    from_above = edges = shifted(downward, 1)
    kernel = functools.partial(upper, high, True, True)
    vectors, upward = step(kernel, UP, (), True, vectors, *also)
    from_below = shifted(upward, -1)
    for sweep in range(0, sweeps, 2):
        more = sweep + 2 < sweeps
        place = 2 if sweep == 2 else 0
        low = [(sweep, {4: 3}), (sweep + 1, {2: 1, 3: 2, 4: 3})]
        high = [(sweep, {0: place}), (sweep + 1, {0: place + 1, 1: 0})]
        if more:
            low.append((sweep + 2, {3: 2}))
            high.append((sweep + 2, {1: 0, 2: 1}))
        ready = prepare(low, *fixed)
        also = prepare(high, *fixed, edges)
        sent = [k for k in (sweep + ahead, sweep + ahead + 1) if k < sweeps] if more else None
        kernel = functools.partial(lower, low, sent, False)
        message = (down_rows(len(sent)), COLS) if more else None
        done = step(kernel, message, (UP,), True, vectors, *ready, packed, from_below)
        vectors = done[0]
        if more:
            later = shifted(done[1], 1)
        kernel = functools.partial(upper, high, more, False)
        message = UP if more else None
        done = step(kernel, message, ((BAND, COLS),), True, vectors, *also, from_above)
        vectors = done[0]
        if more:
            from_below = shifted(done[1], -1)
            edges = edges if sweep == 0 else from_above
            from_above = later
    return final(vectors, panel, row_sum(project(panel, vectors)))


def solution(mesh):
    in_specs = (
        P(),
        P(None, "row"),
        P("col", "row", None, None),
        P("col", "row", None, None),
        P("row", None),
        P("row", "col"),
    )
    out_specs = P("row", "col")
    return jax.shard_map(body, mesh=mesh, in_specs=in_specs, out_specs=out_specs, check_vma=False)
```
